32 devices in a mesh: row: 4 (over z), col: 8 (over y, x, core).
Axes of the slice: x: 2, y: 2, z: 4, core: 2. Of those that a mesh axis runs over, the one named last changes fastest.
Arguments:
- fine_residual: bfloat16 [16, 524288], P(None, ('row', 'col')), may hold values from -6 to 6
- tiles_one: bfloat16 [8192, 128, 128], P(('row', 'col')), may hold values from -0.1875 to 0.1875
- pointers_one: int32 [4128], P(('row', 'col')), may hold values from 0 to 256, as said below
- columns_one: int32 [8192], P(('row', 'col')), may hold values from 0 to 1023, as said below
- points_one: int32 [131072], P(('col', 'row')), may hold values from 0 to 16383, as said below
- tiles_two: bfloat16 [4096, 128, 128], P(('row', 'col')), may hold values from -0.125 to 0.125
- pointers_two: int32 [2080], P(('row', 'col')), may hold values from 0 to 128, as said below
- columns_two: int32 [4096], P(('row', 'col')), may hold values from 0 to 127
- points_two: int32 [32768], P(('row', 'col')), may hold values from 0 to 4095, as said below
- tiles_three: bfloat16 [512, 128, 128], P(('row', 'col')), may hold values from -0.1875 to 0.1875
- pointers_three: int32 [288], P(('row', 'col')), may hold values from 0 to 16, as said below
- columns_three: int32 [512], P(('row', 'col')), may hold values from 0 to 63
- points_three: int32 [8192], P(('col', 'row')), may hold values from 0 to 1023, as said below
Outputs:
- coarse_one: bfloat16 [16, 131072], P(None, ('col', 'row'))
- coarse_two: bfloat16 [16, 32768], P(None, ('row', 'col'))
- coarse_three: bfloat16 [16, 8192], P(None, ('col', 'row'))
The draws below stay inside these ranges and needn't reach their ends.
Inputs may be any that keep to these rules, and one draw needn't show every extreme that they name: `pointers_one`: each tile set's 128 + 1 pointers start at 0 and never fall; the last is that set's live slot count, at most 256; some set has 256 live slots. `pointers_two`: each tile set's 64 + 1 pointers start at 0 and never fall; the last is that set's live slot count, at most 128; some set has 128 live slots. `pointers_three`: each tile set's 8 + 1 pointers start at 0 and never fall; the last is that set's live slot count, at most 16; some set has 16 live slots. `columns_one`: among the live slots of one tile set, at most 32 name block columns with the same quotient by 128; some set reaches 32. `points_one`: values are distinct within each aligned run of 4096 entries. `points_two`: values are distinct within each aligned run of 1024 entries. `points_three`: values are distinct within each aligned run of 256 entries.
All inputs are finite; a program needn't handle non-finite values.
Results may differ from the reference program's by a relative error of at most 0.0057.
Values may be sent and summed in bfloat16 or wider, within the bound.
A program may use at most 128 MiB of HBM per device.

```python
import jax
import jax.numpy as jnp
from jax import lax

TILE_EDGE = 128
VECTORS = 16
PIECE_ROWS = 16384
FINE_ROWS = 524288
COARSE_ONE = 131072
COARSE_TWO = 32768
COARSE_THREE = 8192
BLOCKS_ONE = 128
BLOCKS_TWO = 64
BLOCKS_THREE = 8
SLOTS_ONE = 256
SLOTS_TWO = 128
SLOTS_THREE = 16
FINE_BLOCKS_TWO = 128
FINE_BLOCKS_THREE = 64
PEER_SLOTS = 32
N_ROW = 4
N_COL = 8
DEVICES = 32


def live_counts(level_key, slot_count):
    shifts = jax.random.randint(jax.random.fold_in(level_key, 11), (DEVICES,), 0, 5)
    forced = jax.random.randint(jax.random.fold_in(level_key, 12), (), 0, DEVICES)
    shifts = jnp.where(jnp.arange(DEVICES) == forced, 0, shifts)
    full_slots = jnp.full((DEVICES,), slot_count, jnp.int32)
    return jnp.maximum(jnp.right_shift(full_slots, shifts.astype(jnp.int32)), 1).astype(jnp.int32)


def pointer_table(level_key, slot_count, block_count):
    counts = live_counts(level_key, slot_count)
    block_draw = jax.random.randint(jax.random.fold_in(level_key, 13), (DEVICES, slot_count), 0, block_count)
    positions = jnp.arange(slot_count, dtype=jnp.int32)
    block_draw = jnp.where(positions[None, :] < counts[:, None], block_draw, block_count)
    ordered = jnp.sort(block_draw, axis=1)
    bounds = jnp.arange(block_count + 1, dtype=jnp.int32)
    table = jnp.sum((ordered[:, None, :] < bounds[None, :, None]).astype(jnp.int32), axis=2)
    return table.reshape(-1).astype(jnp.int32)


def point_table(level_key, piece_in, piece_out):
    keys = jax.random.split(level_key, DEVICES)
    chosen = jax.vmap(lambda single: jax.random.permutation(single, piece_in)[:piece_out])(keys)
    return chosen.reshape(-1).astype(jnp.int32)


def draw_pointers_one(key, part):
    return pointer_table(jax.random.fold_in(key, 1), SLOTS_ONE, BLOCKS_ONE)


def draw_pointers_two(key, part):
    return pointer_table(jax.random.fold_in(key, 2), SLOTS_TWO, BLOCKS_TWO)


def draw_pointers_three(key, part):
    return pointer_table(jax.random.fold_in(key, 3), SLOTS_THREE, BLOCKS_THREE)


def draw_columns_one(key, part):
    level_key = jax.random.fold_in(key, 1)
    counts = live_counts(level_key, SLOTS_ONE)
    blocks_peer = PIECE_ROWS // TILE_EDGE
    positions = jnp.arange(SLOTS_ONE, dtype=jnp.int32)
    is_live = positions[None, :] < counts[:, None]
    scores = jax.random.randint(jax.random.fold_in(key, 21), (DEVICES, SLOTS_ONE), 0, 1 << 20) * SLOTS_ONE + positions[None, :]
    scores = jnp.where(is_live, scores, scores + (1 << 30))
    rank_order = jnp.argsort(scores, axis=1)
    hot_rank = jnp.argsort(rank_order, axis=1)
    hot_take = jnp.minimum(counts, PEER_SLOTS)
    is_hot = hot_rank < hot_take[:, None]
    hot_peer = jax.random.randint(jax.random.fold_in(key, 22), (DEVICES,), 0, N_COL)
    base_list = jnp.arange((N_COL - 1) * PEER_SLOTS, dtype=jnp.int32) % (N_COL - 1)
    other_keys = jax.random.split(jax.random.fold_in(key, 23), DEVICES)
    others = jax.vmap(lambda single: jax.random.permutation(single, base_list))(other_keys)
    other_rank = jnp.cumsum(1 - is_hot.astype(jnp.int32), axis=1) - 1
    other_rank = jnp.clip(other_rank, 0, (N_COL - 1) * PEER_SLOTS - 1)
    other_choice = jnp.take_along_axis(others, other_rank, axis=1)
    owner_peer = jnp.where(is_hot, hot_peer[:, None], (hot_peer[:, None] + 1 + other_choice) % N_COL)
    offsets = jax.random.randint(jax.random.fold_in(key, 24), (DEVICES, SLOTS_ONE), 0, blocks_peer)
    return (owner_peer * blocks_peer + offsets).reshape(-1).astype(jnp.int32)


def draw_points_one(key, part):
    return point_table(jax.random.fold_in(key, 31), PIECE_ROWS, PIECE_ROWS // 4)


def draw_points_two(key, part):
    return point_table(jax.random.fold_in(key, 32), PIECE_ROWS // 4, PIECE_ROWS // 16)


def draw_points_three(key, part):
    return point_table(jax.random.fold_in(key, 33), PIECE_ROWS // 16, PIECE_ROWS // 64)


def plant(result, own_key, least, largest):
    dims = result.shape
    spot = [jax.random.randint(jax.random.fold_in(own_key, axis), (), 0, dims[axis]) for axis in range(len(dims))]
    result = result.at[tuple(spot)].set(least)
    longest = dims.index(max(dims))
    spot[longest] = (spot[longest] + 1) % dims[longest]
    return result.at[tuple(spot)].set(largest)


def block_scale(rng, extent, cuts, low, high):
    def one(position, blocks):
        draws = jax.random.uniform(jax.random.fold_in(jax.random.fold_in(rng, 6), position), (blocks,), jnp.float32, low / len(cuts), high / len(cuts))
        return jnp.repeat(jnp.exp(draws), extent[position] // blocks).reshape((-1,) + (1,) * (len(extent) - position - 1))

    level = one(*cuts[0])
    for cut in cuts[1:]:
        level = level * one(*cut)
    return level


def gaussian(rng, shape, deviation, most, pieces=(), kind=jnp.bfloat16):
    array = jax.random.normal(rng, shape, jnp.float32) * deviation
    if len(pieces) > 0:
        array = block_scale(rng, shape, pieces, -0.22, 0.18) * array
    return jnp.clip(array, min=-most, max=most).astype(kind)


def setup_inputs(seed: int = 0) -> dict:
    arg_keys = jax.random.split(jax.random.key(seed), 14)
    return {
        "fine_residual": gaussian(arg_keys[0], (VECTORS, FINE_ROWS), 1.0, 6.0, ((1, 32),)),
        "tiles_one": gaussian(arg_keys[1], (DEVICES * SLOTS_ONE, TILE_EDGE, TILE_EDGE), (2 * TILE_EDGE * N_ROW) ** -0.5, 0.1875, ((0, 32),)),
        "pointers_one": draw_pointers_one(jax.random.fold_in(arg_keys[13], 71), 0),
        "columns_one": draw_columns_one(jax.random.fold_in(arg_keys[13], 71), 0),
        "points_one": draw_points_one(jax.random.fold_in(arg_keys[13], 71), 0),
        "tiles_two": gaussian(arg_keys[5], (DEVICES * SLOTS_TWO, TILE_EDGE, TILE_EDGE), (2 * TILE_EDGE * N_COL) ** -0.5, 0.125, ((0, 32),)),
        "pointers_two": draw_pointers_two(jax.random.fold_in(arg_keys[13], 71), 0),
        "columns_two": plant(jax.random.randint(arg_keys[7], (DEVICES * SLOTS_TWO,), 0, FINE_BLOCKS_TWO), jax.random.fold_in(arg_keys[7], 1), 0, FINE_BLOCKS_TWO - 1).astype(jnp.int32),
        "points_two": draw_points_two(jax.random.fold_in(arg_keys[13], 71), 0),
        "tiles_three": gaussian(arg_keys[9], (DEVICES * SLOTS_THREE, TILE_EDGE, TILE_EDGE), (2 * TILE_EDGE * N_ROW) ** -0.5, 0.1875, ((0, 32),)),
        "pointers_three": draw_pointers_three(jax.random.fold_in(arg_keys[13], 71), 0),
        "columns_three": plant(jax.random.randint(arg_keys[11], (DEVICES * SLOTS_THREE,), 0, FINE_BLOCKS_THREE), jax.random.fold_in(arg_keys[11], 1), 0, FINE_BLOCKS_THREE - 1).astype(jnp.int32),
        "points_three": draw_points_three(jax.random.fold_in(arg_keys[13], 71), 0),
    }


def level_tiles(vector, tiles, columns, pointers, slot_count, block_count, fine_size, coarse_size, coarse_total, even_level):
    tile_edge = tiles.shape[1]
    vector_count = vector.shape[0]
    positions = jnp.arange(slot_count, dtype=jnp.int32)

    def one_device(running, device):
        if even_level:
            fine_index = device // N_COL
            coarse_index = device % N_COL
        else:
            fine_index = device % N_COL
            coarse_index = device // N_COL
        my_tiles = lax.dynamic_slice_in_dim(tiles, (device * slot_count).astype(jnp.int32), slot_count, 0).astype(jnp.float32)
        my_columns = lax.dynamic_slice_in_dim(columns, (device * slot_count).astype(jnp.int32), slot_count, 0)
        my_pointers = lax.dynamic_slice_in_dim(pointers, (device * (block_count + 1)).astype(jnp.int32), block_count + 1, 0)
        is_live = positions < my_pointers[block_count]
        finished = jnp.sum((my_pointers[1:][None, :] <= positions[:, None]).astype(jnp.int32), axis=1)
        segment = jnp.where(is_live, finished, block_count).astype(jnp.int32)
        fine_group = lax.dynamic_slice_in_dim(vector, (fine_index * fine_size).astype(jnp.int32), fine_size, 1).astype(jnp.float32)
        blocks = fine_group.reshape(vector_count, fine_size // tile_edge, tile_edge)
        picked = jnp.take(blocks, my_columns, axis=1)
        products = jnp.einsum("sij,vsj->svi", my_tiles, picked, precision=lax.Precision.HIGHEST)
        summed = jax.ops.segment_sum(products, segment, num_segments=block_count + 1)[:block_count]
        part_sum = jnp.transpose(summed, (1, 0, 2)).reshape(vector_count, coarse_size)
        offset = (coarse_index * coarse_size).astype(jnp.int32)
        current = lax.dynamic_slice_in_dim(running, offset, coarse_size, 1)
        return lax.dynamic_update_slice_in_dim(running, current + part_sum, offset, 1), None

    initial = jnp.zeros((vector_count, coarse_total), jnp.float32)
    running, unused = lax.scan(one_device, initial, jnp.arange(DEVICES, dtype=jnp.int32))
    return running


def point_rows(points, piece_in, piece_out, even_level):
    piece_index = jnp.arange(points.shape[0], dtype=jnp.int32) // piece_out
    if even_level:
        grid_row = piece_index % N_ROW
        grid_col = piece_index // N_ROW
        source = grid_row * N_COL + grid_col
    else:
        grid_row = piece_index // N_COL
        grid_col = piece_index % N_COL
        source = grid_col * N_ROW + grid_row
    return (source * piece_in + points).astype(jnp.int32)


def restrict(vector, tiles, columns, pointers, points, slot_count, block_count, fine_size, coarse_size, coarse_total, piece_in, even_level):
    running = level_tiles(vector, tiles, columns, pointers, slot_count, block_count, fine_size, coarse_size, coarse_total, even_level)
    fine_point = point_rows(points, piece_in, coarse_total // DEVICES, even_level)
    injected = jnp.take(vector, fine_point, axis=1).astype(jnp.float32)
    return (running + injected).astype(jnp.bfloat16)


def reference(fine_residual, tiles_one, pointers_one, columns_one, points_one, tiles_two, pointers_two, columns_two, points_two, tiles_three, pointers_three, columns_three, points_three):
    coarse_one = restrict(fine_residual, tiles_one, columns_one, pointers_one, points_one, SLOTS_ONE, BLOCKS_ONE, FINE_ROWS // N_ROW, COARSE_ONE // N_COL, COARSE_ONE, PIECE_ROWS, True)
    coarse_two = restrict(coarse_one, tiles_two, columns_two, pointers_two, points_two, SLOTS_TWO, BLOCKS_TWO, COARSE_ONE // N_COL, COARSE_TWO // N_ROW, COARSE_TWO, PIECE_ROWS // 4, False)
    coarse_three = restrict(coarse_two, tiles_three, columns_three, pointers_three, points_three, SLOTS_THREE, BLOCKS_THREE, COARSE_TWO // N_ROW, COARSE_THREE // N_COL, COARSE_THREE, PIECE_ROWS // 16, True)
    return (coarse_one, coarse_two, coarse_three)
```

```python
import functools

import jax
import jax.numpy as jnp
from jax import lax
from jax.experimental import pallas as pl
from jax.experimental.pallas import tpu as pltpu
from jax.sharding import PartitionSpec as P


def split_blocks(piece, edge):
    vectors = piece.shape[0]
    return jnp.transpose(piece.reshape(vectors, piece.shape[1] // edge, edge), (1, 0, 2))


def join_blocks(blocks):
    return jnp.transpose(blocks, (1, 0, 2)).reshape(blocks.shape[1], blocks.shape[0] * blocks.shape[2])


def restrict_kernel(step_slots, batch, index_ref, segment_ref, tiles_ref, source_ref, out_ref, total):
    step = pl.program_id(0)
    blocks = out_ref.shape[0]

    @pl.when(step == 0)
    def _():
        total[...] = jnp.zeros_like(total)

    def some(part, carry):
        first = part * batch
        products = []
        for i in range(batch):
            block = source_ref[index_ref[step * step_slots + first + i]]
            products.append(
                lax.dot_general(
                    block,
                    tiles_ref[first + i],
                    (((1,), (1,)), ((), ())),
                    preferred_element_type=jnp.float32,
                )
            )
        for i in range(batch):
            row = segment_ref[step * step_slots + first + i]
            total[row] = total[row] + products[i]
        return carry

    lax.fori_loop(0, step_slots // batch, some, 0)

    @pl.when(step == pl.num_programs(0) - 1)
    def _():
        out_ref[...] = total[:blocks].astype(out_ref.dtype)


def restrict(tiles, source, index, segment, blocks):
    slots, edge, _ = tiles.shape
    vectors = source.shape[1]
    step_slots = min(slots, 64)
    batch = min(step_slots, 8)
    return pl.pallas_call(
        functools.partial(restrict_kernel, step_slots, batch),
        grid_spec=pltpu.PrefetchScalarGridSpec(
            num_scalar_prefetch=2,
            grid=(slots // step_slots,),
            in_specs=[
                pl.BlockSpec((step_slots, edge, edge), lambda s, a, b: (s, 0, 0)),
                pl.BlockSpec(memory_space=pltpu.VMEM),
            ],
            out_specs=pl.BlockSpec(memory_space=pltpu.VMEM),
            scratch_shapes=[pltpu.VMEM((blocks + 1, vectors, edge), jnp.float32)],
        ),
        out_shape=jax.ShapeDtypeStruct((blocks, vectors, edge), jnp.bfloat16),
        cost_estimate=pl.CostEstimate(
            flops=2 * slots * vectors * edge * edge, bytes_accessed=2 * tiles.size, transcendentals=0
        ),
        name="restrict",
    )(index, segment, tiles, source)


def points_kernel(group, unroll, points_ref, source_ref, out_ref):
    chunks, vectors, edge = out_ref.shape
    blocks = source_ref.shape[0]

    def one_group(number, carry):
        lanes, owners = [], []
        for i in range(group):
            points = jnp.broadcast_to(points_ref[number * group + i], (vectors, edge))
            lanes.append(points % edge)
            owners.append(points // edge)

        def some(part, found):
            found = list(found)
            for k in range(unroll):
                j = part * unroll + k
                block = source_ref[j].astype(jnp.float32)
                for i in range(group):
                    picked = jnp.take_along_axis(block, lanes[i], axis=1, mode="promise_in_bounds")
                    found[i] = jnp.where(owners[i] == j, picked, found[i])
            return tuple(found)

        zero = jnp.zeros((vectors, edge), jnp.float32)
        found = lax.fori_loop(0, blocks // unroll, some, (zero,) * group)
        for i in range(group):
            out_ref[number * group + i] = found[i].astype(out_ref.dtype)
        return carry

    lax.fori_loop(0, chunks // group, one_group, 0)


def pick_points(points, source):
    blocks, vectors, edge = source.shape
    chunks = points.shape[0] // edge
    return pl.pallas_call(
        functools.partial(points_kernel, min(chunks, 4), min(blocks, 8)),
        in_specs=[pl.BlockSpec(memory_space=pltpu.VMEM)] * 2,
        out_specs=pl.BlockSpec(memory_space=pltpu.VMEM),
        out_shape=jax.ShapeDtypeStruct((chunks, vectors, edge), source.dtype),
        cost_estimate=pl.CostEstimate(
            flops=8 * chunks * blocks * vectors * edge, bytes_accessed=source.size * 2, transcendentals=0
        ),
        name="points",
    )(points.reshape(chunks, 1, edge), source)


def segments(pointers, slots):
    blocks = pointers.shape[0] - 1
    positions = jnp.arange(slots, dtype=jnp.int32)
    finished = jnp.sum((pointers[1:][None, :] <= positions[:, None]).astype(jnp.int32), axis=1)
    return jnp.where(positions < pointers[blocks], finished, blocks)


def own_sum(partial, injected, axis):
    peers = lax.axis_size(axis)
    blocks = partial.shape[0] // peers
    pieces = partial.reshape((peers, blocks) + partial.shape[1:])
    arrived = lax.all_to_all(pieces, axis, split_axis=0, concat_axis=0, tiled=True)
    summed = jnp.sum(arrived.astype(jnp.float32), axis=0) + injected.astype(jnp.float32)
    return summed.astype(jnp.bfloat16)


def on_device(
    fine_residual,
    tiles_one,
    pointers_one,
    columns_one,
    points_one,
    tiles_two,
    pointers_two,
    columns_two,
    points_two,
    tiles_three,
    pointers_three,
    columns_three,
    points_three,
):
    edge = tiles_one.shape[1]
    slots = tiles_one.shape[0]
    blocks_one = pointers_one.shape[0] - 1
    peers = lax.axis_size("col")
    per_peer = slots // peers
    blocks_peer = fine_residual.shape[1] // edge
    positions = jnp.arange(slots, dtype=jnp.int32)
    live = positions < pointers_one[blocks_one]
    owner = columns_one // blocks_peer
    within = columns_one % blocks_peer
    same = (owner[:, None] == owner[None, :]) & (positions[None, :] < positions[:, None])
    rank = jnp.sum(same.astype(jnp.int32), axis=1)
    target = jnp.where(live, owner * per_peer + rank, slots)
    hits = target[None, :] == positions[:, None]
    requests = jnp.sum(jnp.where(hits, within[None, :], 0), axis=1).reshape(peers, per_peer)
    asked = lax.all_to_all(requests, "col", split_axis=0, concat_axis=0, tiled=True)
    own_blocks = split_blocks(fine_residual, edge)
    found = jnp.take(own_blocks, asked.reshape(-1), axis=0, mode="clip")
    found = found.reshape((peers, per_peer) + found.shape[1:])
    replies = lax.all_to_all(found, "col", split_axis=0, concat_axis=0, tiled=True)
    replies = replies.reshape((slots,) + replies.shape[2:])
    injected = pick_points(points_one, own_blocks)
    partial = restrict(
        tiles_one, replies, jnp.minimum(target, slots - 1), segments(pointers_one, slots), blocks_one
    )
    coarse_one = own_sum(partial, injected, "row")
    group = lax.all_gather(coarse_one, "row", axis=0, tiled=True)
    injected = pick_points(points_two, coarse_one)
    partial = restrict(
        tiles_two, group, columns_two, segments(pointers_two, tiles_two.shape[0]), pointers_two.shape[0] - 1
    )
    coarse_two = own_sum(partial, injected, "col")
    group = lax.all_gather(coarse_two, "col", axis=0, tiled=True)
    injected = pick_points(points_three, coarse_two)
    partial = restrict(
        tiles_three,
        group,
        columns_three,
        segments(pointers_three, tiles_three.shape[0]),
        pointers_three.shape[0] - 1,
    )
    coarse_three = own_sum(partial, injected, "row")
    return (join_blocks(coarse_one), join_blocks(coarse_two), join_blocks(coarse_three))


def solution(mesh):
    placed = (
        P(None, ("row", "col")),
        P(("row", "col"), None, None),
        P(("row", "col")),
        P(("row", "col")),
        P(("col", "row")),
        P(("row", "col"), None, None),
        P(("row", "col")),
        P(("row", "col")),
        P(("row", "col")),
        P(("row", "col"), None, None),
        P(("row", "col")),
        P(("row", "col")),
        P(("col", "row")),
    )
    return jax.shard_map(
        on_device,
        mesh=mesh,
        in_specs=placed,
        out_specs=(P(None, ("col", "row")), P(None, ("row", "col")), P(None, ("col", "row"))),
        check_vma=False,
    )
```

```python
import functools

import jax
import jax.numpy as jnp
from jax import lax
from jax.experimental import pallas as pl
from jax.experimental.pallas import tpu as pltpu
from jax.sharding import PartitionSpec as P


def split_blocks(piece, edge):
    vectors = piece.shape[0]
    return jnp.transpose(piece.reshape(vectors, piece.shape[1] // edge, edge), (1, 0, 2))


def join_blocks(blocks):
    return jnp.transpose(blocks, (1, 0, 2)).reshape(blocks.shape[1], blocks.shape[0] * blocks.shape[2])


def restrict_kernel(step_slots, batch, index_ref, segment_ref, tiles_ref, source_ref, out_ref, total):
    step = pl.program_id(0)
    blocks, vectors, edge = out_ref.shape

    @pl.when(step == 0)
    def _():
        total[...] = jnp.zeros_like(total)

    def some(part, carry):
        first = part * batch
        products = []
        for i in range(0, batch, 2):
            slot = step * step_slots + first + i
            pair = jnp.concatenate([source_ref[index_ref[slot]], source_ref[index_ref[slot + 1]]], axis=0)
            both = lax.dot_general(
                pair,
                tiles_ref[pl.ds(first + i, 2)].reshape(2 * edge, edge),
                (((1,), (1,)), ((), ())),
                preferred_element_type=jnp.float32,
            )
            products.append(both[:vectors, :edge])
            products.append(both[vectors:, edge:])
        for i in range(batch):
            row = segment_ref[step * step_slots + first + i]
            total[row] = total[row] + products[i]
        return carry

    lax.fori_loop(0, step_slots // batch, some, 0)

    @pl.when(step == pl.num_programs(0) - 1)
    def _():
        out_ref[...] = total[:blocks].astype(out_ref.dtype)


def restrict(tiles, source, index, segment, blocks):
    slots, edge, _ = tiles.shape
    vectors = source.shape[1]
    step_slots = min(slots, 64)
    batch = min(step_slots, 8)
    return pl.pallas_call(
        functools.partial(restrict_kernel, step_slots, batch),
        grid_spec=pltpu.PrefetchScalarGridSpec(
            num_scalar_prefetch=2,
            grid=(slots // step_slots,),
            in_specs=[
                pl.BlockSpec((step_slots, edge, edge), lambda s, a, b: (s, 0, 0)),
                pl.BlockSpec(memory_space=pltpu.VMEM),
            ],
            out_specs=pl.BlockSpec(memory_space=pltpu.VMEM),
            scratch_shapes=[pltpu.VMEM((blocks + 1, vectors, edge), jnp.float32)],
        ),
        out_shape=jax.ShapeDtypeStruct((blocks, vectors, edge), jnp.bfloat16),
        cost_estimate=pl.CostEstimate(
            flops=2 * slots * vectors * edge * edge, bytes_accessed=2 * tiles.size, transcendentals=0
        ),
        name="restrict",
    )(index, segment, tiles, source)


def points_kernel(group, span, points_ref, source_ref, out_ref):
    chunks, vectors, edge = out_ref.shape
    blocks = source_ref.shape[0]

    def one_group(number, carry):
        points = points_ref[number]
        owners = jnp.broadcast_to(points // edge, (vectors, group * edge))
        lanes = jnp.broadcast_to(points % edge, (edge, group * edge))
        spots = lax.broadcasted_iota(jnp.int32, (edge, group * edge), 0)
        pick = (lanes == spots).astype(jnp.float32).astype(jnp.bfloat16)
        found = jnp.zeros((vectors, group * edge), jnp.float32)
        for part in range(blocks // span):
            rows = source_ref[part * span : (part + 1) * span].reshape(span * vectors, edge)
            moved = jnp.dot(rows, pick, preferred_element_type=jnp.float32)
            for k in range(span):
                here = moved[k * vectors : (k + 1) * vectors]
                found = jnp.where(owners == part * span + k, here, found)
        for i in range(group):
            out_ref[number * group + i] = found[:, i * edge : (i + 1) * edge].astype(out_ref.dtype)
        return carry

    lax.fori_loop(0, chunks // group, one_group, 0)


def pick_points(points, source):
    blocks, vectors, edge = source.shape
    chunks = points.shape[0] // edge
    group = min(chunks, 2)
    return pl.pallas_call(
        functools.partial(points_kernel, group, min(blocks, 32)),
        in_specs=[pl.BlockSpec(memory_space=pltpu.VMEM)] * 2,
        out_specs=pl.BlockSpec(memory_space=pltpu.VMEM),
        out_shape=jax.ShapeDtypeStruct((chunks, vectors, edge), source.dtype),
        cost_estimate=pl.CostEstimate(
            flops=8 * chunks * blocks * vectors * edge, bytes_accessed=source.size * 2, transcendentals=0
        ),
        name="points",
    )(points.reshape(chunks // group, 1, group * edge), source)


def segments(pointers, slots):
    blocks = pointers.shape[0] - 1
    positions = jnp.arange(slots, dtype=jnp.int32)
    finished = jnp.sum((pointers[1:][None, :] <= positions[:, None]).astype(jnp.int32), axis=1)
    return jnp.where(positions < pointers[blocks], finished, blocks)


def exchange_kernel(axis, peers, gather, partial_ref, injected_ref, *rest):
    if gather:
        own_ref, group_ref, arrived, sent, landed, sent_own, landed_own = rest
    else:
        own_ref, arrived, sent, landed = rest
    me = lax.axis_index(axis)
    others = [lax.rem(me + k, peers) for k in range(1, peers)]
    barrier = pltpu.get_barrier_semaphore()
    for peer in others:
        pl.semaphore_signal(barrier, inc=1, device_id={axis: peer}, device_id_type=pl.DeviceIdType.MESH)
    pl.semaphore_wait(barrier, peers - 1)

    def copies(source, target, out_sem, in_sem):
        started = []
        for k, peer in enumerate(others):
            copy = pltpu.make_async_remote_copy(
                src_ref=source(peer),
                dst_ref=target(k),
                send_sem=out_sem.at[k],
                recv_sem=in_sem.at[k],
                device_id={axis: peer},
                device_id_type=pl.DeviceIdType.MESH,
            )
            copy.start()
            started.append(copy)
        return started

    started = copies(lambda peer: partial_ref.at[peer], lambda k: arrived.at[k], sent, landed)
    total = partial_ref[me].astype(jnp.float32) + injected_ref[...].astype(jnp.float32)
    for k, copy in enumerate(started):
        copy.wait_recv()
        total = total + arrived[k].astype(jnp.float32)
    own_ref[...] = total.astype(own_ref.dtype)
    if gather:
        again = copies(lambda peer: own_ref, lambda k: group_ref.at[me], sent_own, landed_own)
        group_ref[me] = total.astype(own_ref.dtype)
    for copy in started:
        copy.wait_send()
    if gather:
        for copy in again:
            copy.wait()


def own_sum(partial, injected, axis, number, gather):
    peers = lax.axis_size(axis)
    piece = (partial.shape[0] // peers,) + partial.shape[1:]
    pieces = partial.reshape((peers,) + piece)
    kind = partial.dtype
    shapes = [jax.ShapeDtypeStruct(piece, kind)]
    scratch = [pltpu.VMEM((peers - 1,) + piece, kind)] + [pltpu.SemaphoreType.DMA((peers - 1,))] * 2
    if gather:
        shapes.append(jax.ShapeDtypeStruct((peers,) + piece, kind))
        scratch += [pltpu.SemaphoreType.DMA((peers - 1,))] * 2
    found = pl.pallas_call(
        functools.partial(exchange_kernel, axis, peers, gather),
        in_specs=[pl.BlockSpec(memory_space=pltpu.VMEM)] * 2,
        out_specs=[pl.BlockSpec(memory_space=pltpu.VMEM)] * len(shapes),
        out_shape=shapes,
        scratch_shapes=scratch,
        compiler_params=pltpu.CompilerParams(collective_id=number, has_side_effects=True),
        name="exchange",
    )(pieces, injected)
    if gather:
        return found[0], found[1].reshape(partial.shape)
    return found[0]


def on_device(
    fine_residual,
    tiles_one,
    pointers_one,
    columns_one,
    points_one,
    tiles_two,
    pointers_two,
    columns_two,
    points_two,
    tiles_three,
    pointers_three,
    columns_three,
    points_three,
):
    edge = tiles_one.shape[1]
    slots = tiles_one.shape[0]
    blocks_one = pointers_one.shape[0] - 1
    peers = lax.axis_size("col")
    per_peer = slots // peers
    blocks_peer = fine_residual.shape[1] // edge
    positions = jnp.arange(slots, dtype=jnp.int32)
    live = positions < pointers_one[blocks_one]
    owner = columns_one // blocks_peer
    within = columns_one % blocks_peer
    same = (owner[:, None] == owner[None, :]) & (positions[None, :] < positions[:, None])
    rank = jnp.sum(same.astype(jnp.int32), axis=1)
    target = jnp.where(live, owner * per_peer + rank, slots)
    hits = target[None, :] == positions[:, None]
    requests = jnp.sum(jnp.where(hits, within[None, :], 0), axis=1).reshape(peers, per_peer)
    asked = lax.all_to_all(requests, "col", split_axis=0, concat_axis=0, tiled=True)
    own_blocks = split_blocks(fine_residual, edge)
    found = jnp.take(own_blocks, asked.reshape(-1), axis=0, mode="clip")
    found = found.reshape((peers, per_peer) + found.shape[1:])
    replies = lax.all_to_all(found, "col", split_axis=0, concat_axis=0, tiled=True)
    replies = replies.reshape((slots,) + replies.shape[2:])
    injected = pick_points(points_one, own_blocks)
    partial = restrict(
        tiles_one, replies, jnp.minimum(target, slots - 1), segments(pointers_one, slots), blocks_one
    )
    coarse_one, group = own_sum(partial, injected, "row", 0, True)
    injected = pick_points(points_two, coarse_one)
    partial = restrict(
        tiles_two, group, columns_two, segments(pointers_two, tiles_two.shape[0]), pointers_two.shape[0] - 1
    )
    coarse_two, group = own_sum(partial, injected, "col", 1, True)
    injected = pick_points(points_three, coarse_two)
    partial = restrict(
        tiles_three,
        group,
        columns_three,
        segments(pointers_three, tiles_three.shape[0]),
        pointers_three.shape[0] - 1,
    )
    coarse_three = own_sum(partial, injected, "row", 2, False)
    return (join_blocks(coarse_one), join_blocks(coarse_two), join_blocks(coarse_three))


def solution(mesh):
    placed = (
        P(None, ("row", "col")),
        P(("row", "col"), None, None),
        P(("row", "col")),
        P(("row", "col")),
        P(("col", "row")),
        P(("row", "col"), None, None),
        P(("row", "col")),
        P(("row", "col")),
        P(("row", "col")),
        P(("row", "col"), None, None),
        P(("row", "col")),
        P(("row", "col")),
        P(("col", "row")),
    )
    return jax.shard_map(
        on_device,
        mesh=mesh,
        in_specs=placed,
        out_specs=(P(None, ("col", "row")), P(None, ("row", "col")), P(None, ("col", "row"))),
        check_vma=False,
    )
```

```python
import functools

import jax
import jax.numpy as jnp
from jax import lax
from jax.experimental import pallas as pl
from jax.experimental.pallas import tpu as pltpu
from jax.sharding import PartitionSpec as P


def split_blocks(piece, edge):
    vectors = piece.shape[0]
    return jnp.transpose(piece.reshape(vectors, piece.shape[1] // edge, edge), (1, 0, 2))


def join_blocks(blocks):
    return jnp.transpose(blocks, (1, 0, 2)).reshape(blocks.shape[1], blocks.shape[0] * blocks.shape[2])


def restrict_kernel(step_slots, batch, index_ref, segment_ref, tiles_ref, source_ref, out_ref, total):
    step = pl.program_id(0)
    blocks, vectors, edge = out_ref.shape

    @pl.when(step == 0)
    def _():
        total[...] = jnp.zeros_like(total)

    def some(part, carry):
        first = part * batch
        products = []
        for i in range(0, batch, 2):
            slot = step * step_slots + first + i
            pair = jnp.concatenate([source_ref[index_ref[slot]], source_ref[index_ref[slot + 1]]], axis=0)
            both = lax.dot_general(
                pair,
                tiles_ref[pl.ds(first + i, 2)].reshape(2 * edge, edge),
                (((1,), (1,)), ((), ())),
                preferred_element_type=jnp.float32,
            )
            products.append(both[:vectors, :edge])
            products.append(both[vectors:, edge:])
        for i in range(batch):
            row = segment_ref[step * step_slots + first + i]
            total[row] = total[row] + products[i]
        return carry

    lax.fori_loop(0, step_slots // batch, some, 0)

    @pl.when(step == pl.num_programs(0) - 1)
    def _():
        out_ref[...] = total[:blocks].astype(out_ref.dtype)


def restrict(tiles, source, index, segment, blocks):
    slots, edge, _ = tiles.shape
    vectors = source.shape[1]
    step_slots = min(slots, 64)
    batch = min(step_slots, 8)
    return pl.pallas_call(
        functools.partial(restrict_kernel, step_slots, batch),
        grid_spec=pltpu.PrefetchScalarGridSpec(
            num_scalar_prefetch=2,
            grid=(slots // step_slots,),
            in_specs=[
                pl.BlockSpec((step_slots, edge, edge), lambda s, a, b: (s, 0, 0)),
                pl.BlockSpec(memory_space=pltpu.VMEM),
            ],
            out_specs=pl.BlockSpec(memory_space=pltpu.VMEM),
            scratch_shapes=[pltpu.VMEM((blocks + 1, vectors, edge), jnp.float32)],
        ),
        out_shape=jax.ShapeDtypeStruct((blocks, vectors, edge), jnp.bfloat16),
        cost_estimate=pl.CostEstimate(
            flops=2 * slots * vectors * edge * edge, bytes_accessed=2 * tiles.size, transcendentals=0
        ),
        name="restrict",
    )(index, segment, tiles, source)


def points_kernel(group, span, points_ref, source_ref, out_ref):
    chunks, vectors, edge = out_ref.shape
    blocks = source_ref.shape[0]

    def one_group(number, carry):
        points = points_ref[number]
        owners = jnp.broadcast_to(points // edge, (vectors, group * edge))
        lanes = jnp.broadcast_to(points % edge, (edge, group * edge))
        spots = lax.broadcasted_iota(jnp.int32, (edge, group * edge), 0)
        pick = (lanes == spots).astype(jnp.float32).astype(jnp.bfloat16)
        found = jnp.zeros((vectors, group * edge), jnp.float32)
        for part in range(blocks // span):
            rows = source_ref[part * span : (part + 1) * span].reshape(span * vectors, edge)
            moved = jnp.dot(rows, pick, preferred_element_type=jnp.float32)
            for k in range(span):
                here = moved[k * vectors : (k + 1) * vectors]
                found = jnp.where(owners == part * span + k, here, found)
        for i in range(group):
            out_ref[number * group + i] = found[:, i * edge : (i + 1) * edge].astype(out_ref.dtype)
        return carry

    lax.fori_loop(0, chunks // group, one_group, 0)


def pick_points(points, source):
    blocks, vectors, edge = source.shape
    chunks = points.shape[0] // edge
    group = min(chunks, 2)
    return pl.pallas_call(
        functools.partial(points_kernel, group, min(blocks, 32)),
        in_specs=[pl.BlockSpec(memory_space=pltpu.VMEM)] * 2,
        out_specs=pl.BlockSpec(memory_space=pltpu.VMEM),
        out_shape=jax.ShapeDtypeStruct((chunks, vectors, edge), source.dtype),
        cost_estimate=pl.CostEstimate(
            flops=8 * chunks * blocks * vectors * edge, bytes_accessed=source.size * 2, transcendentals=0
        ),
        name="points",
    )(points.reshape(chunks // group, 1, group * edge), source)


def segments(pointers, slots):
    positions = jnp.arange(slots, dtype=jnp.int32)
    return jnp.sum((pointers[None, :] <= positions[:, None]).astype(jnp.int32), axis=1) - 1


def exchange_kernel(axis, peers, gather, partial_ref, injected_ref, *rest):
    if gather:
        own_ref, group_ref, arrived, sent, landed, sent_own, landed_own = rest
    else:
        own_ref, arrived, sent, landed = rest
    me = lax.axis_index(axis)
    others = [lax.rem(me + k, peers) for k in range(1, peers)]
    barrier = pltpu.get_barrier_semaphore()
    for peer in others:
        pl.semaphore_signal(barrier, inc=1, device_id={axis: peer}, device_id_type=pl.DeviceIdType.MESH)
    pl.semaphore_wait(barrier, peers - 1)

    chunks = sent.shape[0]
    size = injected_ref.shape[0] // chunks
    parts = [pl.ds(h * size, size) for h in range(chunks)]

    def copies(source, target, out_sem, in_sem, h):
        started = []
        for k, peer in enumerate(others):
            copy = pltpu.make_async_remote_copy(
                src_ref=source(peer),
                dst_ref=target(k),
                send_sem=out_sem.at[h, k],
                recv_sem=in_sem.at[h, k],
                device_id={axis: peer},
                device_id_type=pl.DeviceIdType.MESH,
            )
            copy.start()
            started.append(copy)
        return started

    first, again = [], []
    for h, part in enumerate(parts):
        first.append(
            copies(lambda peer: partial_ref.at[peer, part], lambda k: arrived.at[k, part], sent, landed, h)
        )
    for h, part in enumerate(parts):
        total = partial_ref[me, part].astype(jnp.float32) + injected_ref[part].astype(jnp.float32)
        for k, copy in enumerate(first[h]):
            copy.wait_recv()
            total = total + arrived[k, part].astype(jnp.float32)
        own_ref[part] = total.astype(own_ref.dtype)
        if gather:
            again += copies(
                lambda peer: own_ref.at[part], lambda k: group_ref.at[me, part], sent_own, landed_own, h
            )
            group_ref[me, part] = total.astype(own_ref.dtype)
    for started in first:
        for copy in started:
            copy.wait_send()
    for copy in again:
        copy.wait()


def own_sum(partial, injected, axis, number, gather):
    peers = lax.axis_size(axis)
    piece = (partial.shape[0] // peers,) + partial.shape[1:]
    pieces = partial.reshape((peers,) + piece)
    kind = partial.dtype
    chunks = 2 if piece[0] % 32 == 0 else 1
    shapes = [jax.ShapeDtypeStruct(piece, kind)]
    scratch = [pltpu.VMEM((peers - 1,) + piece, kind)] + [pltpu.SemaphoreType.DMA((chunks, peers - 1))] * 2
    if gather:
        shapes.append(jax.ShapeDtypeStruct((peers,) + piece, kind))
        scratch += [pltpu.SemaphoreType.DMA((chunks, peers - 1))] * 2
    found = pl.pallas_call(
        functools.partial(exchange_kernel, axis, peers, gather),
        in_specs=[pl.BlockSpec(memory_space=pltpu.VMEM)] * 2,
        out_specs=[pl.BlockSpec(memory_space=pltpu.VMEM)] * len(shapes),
        out_shape=shapes,
        scratch_shapes=scratch,
        compiler_params=pltpu.CompilerParams(collective_id=number, has_side_effects=True),
        name="exchange",
    )(pieces, injected)
    if gather:
        return found[0], found[1].reshape(partial.shape)
    return found[0]


def on_device(
    fine_residual,
    tiles_one,
    pointers_one,
    columns_one,
    points_one,
    tiles_two,
    pointers_two,
    columns_two,
    points_two,
    tiles_three,
    pointers_three,
    columns_three,
    points_three,
):
    edge = tiles_one.shape[1]
    slots = tiles_one.shape[0]
    blocks_one = pointers_one.shape[0] - 1
    peers = lax.axis_size("col")
    per_peer = slots // peers
    blocks_peer = fine_residual.shape[1] // edge
    positions = jnp.arange(slots, dtype=jnp.int32)
    segment_one = segments(pointers_one, slots)
    live = segment_one < blocks_one
    owner = columns_one // blocks_peer
    within = columns_one % blocks_peer
    same = (owner[:, None] == owner[None, :]) & (positions[None, :] < positions[:, None])
    rank = jnp.sum(same.astype(jnp.int32), axis=1)
    target = jnp.where(live, owner * per_peer + rank, slots)
    hits = target[None, :] == positions[:, None]
    requests = jnp.sum(jnp.where(hits, within[None, :], 0), axis=1).reshape(peers, per_peer)
    asked = lax.all_to_all(requests, "col", split_axis=0, concat_axis=0, tiled=True)
    own_blocks = split_blocks(fine_residual, edge)
    found = jnp.take(own_blocks, asked.reshape(-1), axis=0, mode="clip")
    found = found.reshape((peers, per_peer) + found.shape[1:])
    replies = lax.all_to_all(found, "col", split_axis=0, concat_axis=0, tiled=True)
    replies = replies.reshape((slots,) + replies.shape[2:])
    injected = pick_points(points_one, own_blocks)
    partial = restrict(
        tiles_one, replies, jnp.minimum(target, slots - 1), segment_one, blocks_one
    )
    coarse_one, group = own_sum(partial, injected, "row", 0, True)
    injected = pick_points(points_two, coarse_one)
    partial = restrict(
        tiles_two, group, columns_two, segments(pointers_two, tiles_two.shape[0]), pointers_two.shape[0] - 1
    )
    coarse_two, group = own_sum(partial, injected, "col", 1, True)
    injected = pick_points(points_three, coarse_two)
    partial = restrict(
        tiles_three,
        group,
        columns_three,
        segments(pointers_three, tiles_three.shape[0]),
        pointers_three.shape[0] - 1,
    )
    coarse_three = own_sum(partial, injected, "row", 2, False)
    return (join_blocks(coarse_one), join_blocks(coarse_two), join_blocks(coarse_three))


def solution(mesh):
    placed = (
        P(None, ("row", "col")),
        P(("row", "col"), None, None),
        P(("row", "col")),
        P(("row", "col")),
        P(("col", "row")),
        P(("row", "col"), None, None),
        P(("row", "col")),
        P(("row", "col")),
        P(("row", "col")),
        P(("row", "col"), None, None),
        P(("row", "col")),
        P(("row", "col")),
        P(("col", "row")),
    )
    return jax.shard_map(
        on_device,
        mesh=mesh,
        in_specs=placed,
        out_specs=(P(None, ("col", "row")), P(None, ("row", "col")), P(None, ("col", "row"))),
        check_vma=False,
    )
```
